32 devices in a mesh: pts: 32 (over z, y, x, core).
Axes of the slice: x: 2, y: 2, z: 4, core: 2. Of those that a mesh axis runs over, the one named last changes fastest.
Arguments:
- points: bfloat16 [16384, 64], P('pts'), may hold values from -10 to 10, as said below
- targets: float32 [16384], P('pts'), may hold values from -6 to 6
- ridge_weight: float32 [], replicated, may hold values from 0.5 to 4
Outputs:
- coefficients: float32 [16384], P('pts')
- residual: float32 [16384], P('pts')
The draws below stay inside these ranges and needn't reach their ends.
Inputs may be any that keep to these rules, and one draw needn't show every extreme that they name: `points`: each point lies near one of 341 cluster centres; every coordinate is within -10 and 10.
All inputs are finite; a program needn't handle non-finite values.
Results may differ from the reference program's by a relative error of at most 0.005.
Values may be sent and summed in bfloat16 or wider, within the bound.
A program may use at most 192 MiB of HBM per device.

```python
import math
import jax
import jax.numpy as jnp
from jax import lax

D = 64
PTS_DEV = 512
ITERS = 2
NPTS = 16384
CLUSTERS = 341


def draw_points(key, part):
    key_centre = jax.random.fold_in(key, 11)
    key_member = jax.random.fold_in(key, 12)
    key_noise = jax.random.fold_in(key, 13)
    centres = 0.5 * jax.random.truncated_normal(key_centre, -4.0, 4.0, (CLUSTERS, D), jnp.float32)
    members = jax.random.randint(key_member, (NPTS,), 0, CLUSTERS)
    noise = 0.5 * jax.random.truncated_normal(key_noise, -4.0, 4.0, (NPTS, D), jnp.float32)
    return (centres[members] + noise).astype(jnp.bfloat16)


def level_of(rng, dims, pieces, smallest, high):
    def one(axis_at, shards_of):
        steps = jax.random.uniform(jax.random.fold_in(jax.random.fold_in(rng, 6), axis_at), (shards_of,), jnp.float32, smallest / len(pieces), high / len(pieces))
        return jnp.repeat(jnp.exp(steps), dims[axis_at] // shards_of).reshape((-1,) + (1,) * (len(dims) - axis_at - 1))

    factor_of = one(*pieces[0])
    for cut in pieces[1:]:
        factor_of = factor_of * one(*cut)
    return factor_of


def normal_values(own_key, dims, scale, bound, split=(), kind=jnp.bfloat16):
    result = scale * jax.random.normal(own_key, dims, jnp.float32)
    if split:
        result = result * level_of(own_key, dims, split, -0.22, 0.18)
    return jnp.clip(result, -bound, bound).astype(kind)


def setup_inputs(seed: int = 0) -> dict:
    arg_keys = jax.random.split(jax.random.key(seed), 4)
    points = draw_points(jax.random.fold_in(arg_keys[3], 71), 0)
    targets = normal_values(arg_keys[1], (NPTS,), 1.0, 6.0, ((0, 32),), jnp.float32)
    ridge_weight = jnp.clip(jnp.exp(jax.random.uniform(arg_keys[2], (), jnp.float32, math.log(0.5), math.log(4.0))), 0.5, 4.0)
    return dict(points=points, targets=targets, ridge_weight=ridge_weight)


def reference(points, targets, ridge_weight):
    inverse_width = 1.0 / D
    widened = points.astype(jnp.float32)
    squared = jnp.sum(widened * widened, axis=1)
    blocks = points.reshape(NPTS // PTS_DEV, PTS_DEV, D)
    block_norms = squared.reshape(NPTS // PTS_DEV, PTS_DEV)

    def apply_operator(vector):
        vector_low = vector.astype(jnp.bfloat16)

        def tile_product(operands):
            tile_rows, tile_norms = operands
            cross_term = jnp.dot(tile_rows, points.T, preferred_element_type=jnp.float32)
            distance = tile_norms[:, None] + squared[None, :] - 2.0 * cross_term
            kernel = jnp.exp(-inverse_width * distance).astype(jnp.bfloat16)
            return jnp.dot(kernel, vector_low, preferred_element_type=jnp.float32)

        summed = lax.map(tile_product, (blocks, block_norms)).reshape(NPTS)
        return summed + ridge_weight * vector

    coefficients = jnp.zeros_like(targets)
    residual = targets
    direction = targets
    norm_now = jnp.sum(residual * residual)
    for iteration in range(ITERS):
        applied = apply_operator(direction)
        step_size = norm_now / jnp.sum(direction * applied)
        coefficients = coefficients + step_size * direction
        residual = residual - step_size * applied
        norm_next = jnp.sum(residual * residual)
        direction = residual + (norm_next / norm_now) * direction
        norm_now = norm_next
    return coefficients, residual
```

```python
import functools

import jax
import jax.numpy as jnp
from jax import lax
from jax.experimental import pallas as pl
from jax.experimental.pallas import tpu as pltpu
from jax.sharding import PartitionSpec as P

F32 = jnp.float32
BF16 = jnp.bfloat16
KEEP_BYTES = 40 * 1024 * 1024


def kernel(n, dim, keep, pts, tgt, ridge, coef_out, res_out, mine, blocks, t_all, w_all,
           c_all, r_a, r_b, kt, sem_ts, sem_tr, sem_ps, sem_pr, sem_fs, sem_fr, sem_ws,
           sem_wr, sem_cs, sem_cr):
    me = lax.axis_index("pts")
    half_n = n // 2
    core = lax.rem(me, 2)
    partner = me + 1 - 2 * core
    local = tgt.shape[1]
    half = local // 2
    wide = 2 * dim

    def same(k):
        return lax.rem(me + 2 * k, n)

    def other(k):
        d = lax.rem(me + 2 * k, n)
        return d + 1 - 2 * lax.rem(d, 2)

    barrier = pltpu.get_barrier_semaphore()

    @pl.loop(1, n)
    def _(k):
        pl.semaphore_signal(barrier, inc=1, device_id=(lax.rem(me + k, n),),
                            device_id_type=pl.DeviceIdType.MESH)

    own = pts[...].astype(F32)
    packed = jnp.concatenate([own[:half], own[half:]], axis=1).astype(BF16)
    mine[...] = packed
    own_t = own.T
    s_row = jnp.sum(own_t * own_t, axis=0, keepdims=True) * (-1.0 / dim)
    s_hi = s_row.astype(BF16).astype(F32)
    s_mid = (s_row - s_hi).astype(BF16).astype(F32)
    s_lo = s_row - s_hi - s_mid
    rows = lax.broadcasted_iota(jnp.int32, (dim, local), 0)
    pieces = jnp.where(rows == 0, s_hi, jnp.where(rows == 1, s_mid, jnp.where(rows == 2, s_lo, 0.0)))
    pieces = pieces.astype(BF16)
    scaled = (own_t * (2.0 / dim)).astype(BF16)
    minus = jnp.full((dim, local), -1.0 / dim, BF16)
    r_a[0:dim] = scaled
    r_a[dim:2 * dim] = minus
    r_a[2 * dim:3 * dim] = minus
    r_a[3 * dim:4 * dim] = pieces
    r_b[0:dim] = minus
    r_b[dim:2 * dim] = scaled
    r_b[2 * dim:3 * dim] = pieces
    r_b[3 * dim:4 * dim] = minus

    def send(src, dst, ssem, rsem, dev):
        return pltpu.make_async_remote_copy(
            src_ref=src, dst_ref=dst, send_sem=ssem, recv_sem=rsem,
            device_id=(dev,), device_id_type=pl.DeviceIdType.MESH)

    def t_copy(p, k):
        return send(tgt, t_all.at[p, k], sem_ts.at[p, k], sem_tr.at[p, k], other(k) if p else same(k))

    def w_copy(p, k):
        return send(w_all.at[0, 0], w_all.at[p, k], sem_ws.at[p, k], sem_wr.at[p, k], other(k) if p else same(k))

    def c_copy(p, k):
        return send(c_all.at[0, 0], c_all.at[p, k], sem_cs.at[p, k], sem_cr.at[p, k], other(k) if p else same(k))

    def p_copy(k):
        return send(mine, blocks.at[0, k], sem_ps.at[k], sem_pr.at[k], same(k))

    def f_first():
        return send(mine, blocks.at[1, 0], sem_fs.at[0], sem_fr.at[0], partner)

    def f_copy(k):
        return send(blocks.at[0, k], blocks.at[1, k], sem_fs.at[k], sem_fr.at[k], partner)

    def each(fn):
        fn(1, 0)

        @pl.loop(1, half_n)
        def _(k):
            fn(0, k)
            fn(1, k)

    pl.semaphore_wait(barrier, n - 1)
    f_first().start()

    @pl.loop(1, half_n)
    def _(k):
        p_copy(k).start()

    each(lambda p, k: t_copy(p, k).start())
    t_all[0, 0] = tgt[...]

    lanes = lax.broadcasted_iota(jnp.int32, (half, wide), 1)
    first = lanes < dim
    one = jnp.ones((half, wide), BF16)

    def tile(pb):
        f = pb.astype(F32)
        sq = f * f
        hi = sq.astype(BF16)
        lo = (sq - hi.astype(F32)).astype(BF16)
        hi = pltpu.roll(hi.astype(F32), dim, 1).astype(BF16)
        top = jnp.concatenate([jnp.where(first, pb, hi), jnp.where(first, lo, one)], axis=1)
        bot = jnp.concatenate([jnp.where(first, hi, pb), jnp.where(first, one, lo)], axis=1)
        e_top = jnp.dot(top, r_a[...], preferred_element_type=F32)
        k_top = jnp.exp(e_top).astype(BF16)
        e_bot = jnp.dot(bot, r_b[...], preferred_element_type=F32)
        k_bot = jnp.exp(e_bot).astype(BF16)
        return k_top, k_bot

    def absorb(pb, p, k, vec, acc):
        k_top, k_bot = tile(pb)
        if keep:
            kt[p, k, 0:half] = k_top
            kt[p, k, half:local] = k_bot
        v = vec.astype(BF16)
        acc = acc + jnp.dot(v[:, :half], k_top, preferred_element_type=F32)
        return acc + jnp.dot(v[:, half:], k_bot, preferred_element_type=F32)

    acc = jnp.zeros((1, local), F32)
    acc = absorb(mine[...], 0, 0, tgt[...], acc)
    f_first().wait_recv()
    t_copy(1, 0).wait_recv()
    acc = absorb(blocks[1, 0], 1, 0, t_all[1, 0], acc)

    def step(k, acc):
        p_copy(k).wait_recv()
        f_copy(k).start()
        t_copy(0, k).wait_recv()
        acc = absorb(blocks[0, k], 0, k, t_all[0, k], acc)
        f_copy(k).wait_recv()
        t_copy(1, k).wait_recv()
        return absorb(blocks[1, k], 1, k, t_all[1, k], acc)

    acc = lax.fori_loop(1, half_n, step, acc)
    weight = ridge[0, 0]
    w_all[0, 0] = acc + weight * tgt[...]
    t_whole = t_all[...]
    norm0 = jnp.sum(t_whole * t_whole)
    each(lambda p, k: w_copy(p, k).start())

    f_first().wait_send()

    @pl.loop(1, half_n)
    def _(k):
        p_copy(k).wait_send()
        f_copy(k).wait_send()

    each(lambda p, k: t_copy(p, k).wait_send())
    each(lambda p, k: w_copy(p, k).wait_recv())
    each(lambda p, k: w_copy(p, k).wait_send())
    w_whole = w_all[...]
    step0 = norm0 / jnp.sum(t_whole * w_whole)
    r1 = t_whole - step0 * w_whole
    norm1 = jnp.sum(r1 * r1)
    d1 = r1 + (norm1 / norm0) * t_whole
    t_all[...] = d1

    def again(k, acc):
        for p in (0, 1):
            if keep:
                acc = acc + jnp.dot(t_all[p, k].astype(BF16), kt[p, k], preferred_element_type=F32)
            else:
                acc = absorb(blocks[p, k], p, k, t_all[p, k], acc)
        return acc

    if not keep:
        blocks[0, 0] = mine[...]
    acc = lax.fori_loop(0, half_n, again, jnp.zeros((1, local), F32))
    d_own = t_all[0, 0]
    applied = acc + weight * d_own
    part = jnp.sum(d_own * applied)
    c_all[0, 0] = jnp.full((1, 128), part, F32)
    each(lambda p, k: c_copy(p, k).start())
    each(lambda p, k: c_copy(p, k).wait_recv())
    each(lambda p, k: c_copy(p, k).wait_send())
    curvature = jnp.sum(jnp.sum(c_all[...], axis=(0, 1)), axis=0, keepdims=True)[:, 0:1]
    step1 = norm1 / curvature
    coef_out[...] = step0 * tgt[...] + step1 * d_own
    res_out[...] = tgt[...] - step0 * w_all[0, 0] - step1 * applied


def body(n, points, targets, ridge_weight):
    local, dim = points.shape
    half_n = n // 2
    keep = n * local * local * 2 <= KEEP_BYTES
    kt_shape = (2, half_n, local, local) if keep else (1, 1, 16, 128)
    dma = pltpu.SemaphoreType.DMA
    vec = jax.ShapeDtypeStruct((1, local), F32)
    coef, res = pl.pallas_call(
        functools.partial(kernel, n, dim, keep),
        out_shape=(vec, vec),
        in_specs=[
            pl.BlockSpec(memory_space=pltpu.VMEM),
            pl.BlockSpec(memory_space=pltpu.VMEM),
            pl.BlockSpec(memory_space=pltpu.SMEM),
        ],
        out_specs=(pl.BlockSpec(memory_space=pltpu.VMEM), pl.BlockSpec(memory_space=pltpu.VMEM)),
        scratch_shapes=[
            pltpu.VMEM((local // 2, 2 * dim), BF16),
            pltpu.VMEM((2, half_n, local // 2, 2 * dim), BF16),
            pltpu.VMEM((2, half_n, 1, local), F32),
            pltpu.VMEM((2, half_n, 1, local), F32),
            pltpu.VMEM((2, half_n, 1, 128), F32),
            pltpu.VMEM((4 * dim, local), BF16),
            pltpu.VMEM((4 * dim, local), BF16),
            pltpu.VMEM(kt_shape, BF16),
            dma((2, half_n)), dma((2, half_n)),
            dma((half_n,)), dma((half_n,)),
            dma((half_n,)), dma((half_n,)),
            dma((2, half_n)), dma((2, half_n)),
            dma((2, half_n)), dma((2, half_n)),
        ],
        compiler_params=pltpu.CompilerParams(
            collective_id=0, has_side_effects=True, vmem_limit_bytes=60 * 1024 * 1024),
    )(points, targets.reshape(1, local), ridge_weight.reshape(1, 1))
    return coef.reshape(local), res.reshape(local)


def solution(mesh):
    n = mesh.shape["pts"]
    return jax.shard_map(
        functools.partial(body, n), mesh=mesh,
        in_specs=(P("pts", None), P("pts"), P()),
        out_specs=(P("pts"), P("pts")), check_vma=False)
```

```python
import functools

import jax
import jax.numpy as jnp
from jax import lax
from jax.experimental import pallas as pl
from jax.experimental.pallas import tpu as pltpu
from jax.sharding import PartitionSpec as P

F32 = jnp.float32
BF16 = jnp.bfloat16
KEEP_BYTES = 40 * 1024 * 1024


def kernel(n, dim, keep, pts_hbm, tgt, ridge, coef_out, res_out, pts, blocks, t_all, w_all,
           c_all, r_a, r_b, kt, sem_in, sem_ps, sem_pr, sem_fs, sem_fr, sem_ws,
           sem_wr, sem_gs, sem_gr, sem_cs, sem_cr):
    me = lax.axis_index("pts")
    half_n = n // 2
    stages = half_n.bit_length() - 1
    local = tgt.shape[1]
    half = local // 2
    wide = 2 * dim
    t_rows = local // wide

    def device(p, q):
        d = lax.rem(me + p, 2)
        for s in range(stages):
            bit = half_n >> s
            d = d + lax.rem(me // bit + q // (1 << s), 2) * bit
        return d

    partner = device(1, 0)
    load = pltpu.make_async_copy(pts_hbm, pts, sem_in)
    load.start()
    barrier = pltpu.get_barrier_semaphore()
    for dev in [partner] + [device(0, 1 << s) for s in range(stages)]:
        pl.semaphore_signal(barrier, inc=1, device_id=(dev,), device_id_type=pl.DeviceIdType.MESH)

    target = tgt[...]
    t_hi = target.astype(BF16)
    t_rest = target - t_hi.astype(F32)
    t_mid = t_rest.astype(BF16)
    t_lo = (t_rest - t_mid.astype(F32)).astype(BF16)
    cut = [part.astype(F32)[:, i * wide:(i + 1) * wide] for part in (t_hi, t_mid, t_lo) for i in range(t_rows)]
    pad = -len(cut) % 16
    t_tile = jnp.concatenate(cut + [jnp.zeros((pad, wide), F32)], axis=0).astype(BF16)
    load.wait()
    own = pts[...].astype(F32)
    blocks[0, 0, 0:half] = jnp.concatenate([own[:half], own[half:]], axis=1).astype(BF16)
    blocks[0, 0, half:] = t_tile
    t_all[0, 0] = target
    own_t = own.T
    s_row = jnp.sum(own_t * own_t, axis=0, keepdims=True) * (-1.0 / dim)
    s_hi = s_row.astype(BF16).astype(F32)
    s_mid = (s_row - s_hi).astype(BF16).astype(F32)
    s_lo = s_row - s_hi - s_mid
    rows = lax.broadcasted_iota(jnp.int32, (dim, local), 0)
    pieces = jnp.where(rows == 0, s_hi, jnp.where(rows == 1, s_mid, jnp.where(rows == 2, s_lo, 0.0)))
    pieces = pieces.astype(BF16)
    scaled = (own_t * (2.0 / dim)).astype(BF16)
    minus = jnp.full((dim, local), -1.0 / dim, BF16)
    r_a[0:dim] = scaled
    r_a[dim:2 * dim] = minus
    r_a[2 * dim:3 * dim] = minus
    r_a[3 * dim:4 * dim] = pieces
    r_b[0:dim] = minus
    r_b[dim:2 * dim] = scaled
    r_b[2 * dim:3 * dim] = pieces
    r_b[3 * dim:4 * dim] = minus

    def send(src, dst, ssem, rsem, dev):
        return pltpu.make_async_remote_copy(
            src_ref=src, dst_ref=dst, send_sem=ssem, recv_sem=rsem,
            device_id=(dev,), device_id_type=pl.DeviceIdType.MESH)

    def w_copy(q):
        return send(w_all.at[0, 0], w_all.at[0, q], sem_ws.at[q], sem_wr.at[q], device(0, q))

    def g_copy(q):
        return send(w_all.at[0, q], w_all.at[1, q], sem_gs.at[q], sem_gr.at[q], partner)

    def c_copy(p, q):
        return send(c_all.at[0, 0], c_all.at[p, q], sem_cs.at[p, q], sem_cr.at[p, q], device(p, q))

    def p_copy(q, s):
        to = q + (1 << s)
        return send(blocks.at[0, q], blocks.at[0, to], sem_ps.at[to], sem_pr.at[to], device(0, 1 << s))

    def p_from(q):
        return send(blocks.at[0, 0], blocks.at[0, q], sem_ps.at[q], sem_pr.at[q], partner)

    def f_copy(q):
        return send(blocks.at[0, q], blocks.at[1, q], sem_fs.at[q], sem_fr.at[q], partner)

    def each(fn):
        fn(1, 0)

        @pl.loop(1, half_n)
        def _(q):
            fn(0, q)
            fn(1, q)

    pl.semaphore_wait(barrier, stages + 1)
    for s in reversed(range(stages)):
        p_copy(0, s).start()
    f_copy(0).start()

    lanes = lax.broadcasted_iota(jnp.int32, (half, wide), 1)
    first = lanes < dim
    one = jnp.ones((half, wide), BF16)

    def tile(pb):
        f = pb.astype(F32)
        sq = f * f
        hi = sq.astype(BF16)
        lo = (sq - hi.astype(F32)).astype(BF16)
        hi = pltpu.roll(hi.astype(F32), dim, 1).astype(BF16)
        top = jnp.concatenate([jnp.where(first, pb, hi), jnp.where(first, lo, one)], axis=1)
        bot = jnp.concatenate([jnp.where(first, hi, pb), jnp.where(first, one, lo)], axis=1)
        e_top = jnp.dot(top, r_a[...], preferred_element_type=F32)
        k_top = jnp.exp(e_top).astype(BF16)
        e_bot = jnp.dot(bot, r_b[...], preferred_element_type=F32)
        k_bot = jnp.exp(e_bot).astype(BF16)
        return k_top, k_bot

    def absorb(p, q, vec, acc):
        k_top, k_bot = tile(blocks[p, q, 0:half])
        if keep:
            kt[p, q, 0:half] = k_top
            kt[p, q, half:local] = k_bot
        v = vec.astype(BF16)
        acc = acc + jnp.dot(v[:, :half], k_top, preferred_element_type=F32)
        return acc + jnp.dot(v[:, half:], k_bot, preferred_element_type=F32)

    def unpack(p, q):
        part = blocks[p, q, half:].astype(F32)
        hi, mid, lo = (
            jnp.concatenate([part[i * t_rows + j:i * t_rows + j + 1] for j in range(t_rows)], axis=1)
            for i in range(3))
        vec = hi + mid + lo
        t_all[p, q] = vec
        return vec

    acc = jnp.zeros((1, local), F32)
    acc = absorb(0, 0, target, acc)
    f_copy(0).wait_recv()
    acc = absorb(1, 0, unpack(1, 0), acc)

    def step(q, acc):
        p_from(q).wait_recv()
        for s in reversed(range(stages)):
            @pl.when(q < (1 << s))
            def _():
                p_copy(q, s).start()
        f_copy(q).start()
        acc = absorb(0, q, unpack(0, q), acc)
        f_copy(q).wait_recv()
        return absorb(1, q, unpack(1, q), acc)

    acc = lax.fori_loop(1, half_n, step, acc)
    weight = ridge[0, 0]
    w_all[0, 0] = acc + weight * target
    t_whole = t_all[...]
    norm0 = jnp.sum(t_whole * t_whole)
    g_copy(0).start()

    @pl.loop(1, half_n)
    def _(q):
        w_copy(q).start()

    f_copy(0).wait_send()

    @pl.loop(1, half_n)
    def _(q):
        p_from(q).wait_send()
        f_copy(q).wait_send()

    @pl.loop(1, half_n)
    def _(q):
        w_copy(q).wait_recv()
        g_copy(q).start()

    @pl.loop(1, half_n)
    def _(q):
        w_copy(q).wait_send()

    @pl.loop(0, half_n)
    def _(q):
        g_copy(q).wait()

    w_whole = w_all[...]
    step0 = norm0 / jnp.sum(t_whole * w_whole)
    r1 = t_whole - step0 * w_whole
    norm1 = jnp.sum(r1 * r1)
    d1 = r1 + (norm1 / norm0) * t_whole
    t_all[...] = d1

    def again(q, acc):
        for p in (0, 1):
            if keep:
                acc = acc + jnp.dot(t_all[p, q].astype(BF16), kt[p, q], preferred_element_type=F32)
            else:
                acc = absorb(p, q, t_all[p, q], acc)
        return acc

    acc = lax.fori_loop(0, half_n, again, jnp.zeros((1, local), F32))
    d_own = t_all[0, 0]
    applied = acc + weight * d_own
    part = jnp.sum(d_own * applied)
    c_all[0, 0] = jnp.full((1, 128), part, F32)
    each(lambda p, q: c_copy(p, q).start())
    each(lambda p, q: c_copy(p, q).wait_recv())
    each(lambda p, q: c_copy(p, q).wait_send())
    curvature = jnp.sum(jnp.sum(c_all[...], axis=(0, 1)), axis=0, keepdims=True)[:, 0:1]
    step1 = norm1 / curvature
    coef_out[...] = step0 * target + step1 * d_own
    res_out[...] = target - step0 * w_all[0, 0] - step1 * applied


def body(n, points, targets, ridge_weight):
    local, dim = points.shape
    half_n = n // 2
    keep = n * local * local * 2 <= KEEP_BYTES
    kt_shape = (2, half_n, local, local) if keep else (1, 1, 16, 128)
    t_tile = -(-3 * local // (32 * dim)) * 16
    dma = pltpu.SemaphoreType.DMA
    vec = jax.ShapeDtypeStruct((1, local), F32)
    coef, res = pl.pallas_call(
        functools.partial(kernel, n, dim, keep),
        out_shape=(vec, vec),
        in_specs=[
            pl.BlockSpec(memory_space=pl.ANY),
            pl.BlockSpec(memory_space=pltpu.VMEM),
            pl.BlockSpec(memory_space=pltpu.SMEM),
        ],
        out_specs=(pl.BlockSpec(memory_space=pltpu.VMEM), pl.BlockSpec(memory_space=pltpu.VMEM)),
        scratch_shapes=[
            pltpu.VMEM((local, dim), BF16),
            pltpu.VMEM((2, half_n, local // 2 + t_tile, 2 * dim), BF16),
            pltpu.VMEM((2, half_n, 1, local), F32),
            pltpu.VMEM((2, half_n, 1, local), F32),
            pltpu.VMEM((2, half_n, 1, 128), F32),
            pltpu.VMEM((4 * dim, local), BF16),
            pltpu.VMEM((4 * dim, local), BF16),
            pltpu.VMEM(kt_shape, BF16),
            dma,
            dma((half_n,)), dma((half_n,)),
            dma((half_n,)), dma((half_n,)),
            dma((half_n,)), dma((half_n,)),
            dma((half_n,)), dma((half_n,)),
            dma((2, half_n)), dma((2, half_n)),
        ],
        compiler_params=pltpu.CompilerParams(
            collective_id=0, has_side_effects=True, vmem_limit_bytes=60 * 1024 * 1024),
    )(points, targets.reshape(1, local), ridge_weight.reshape(1, 1))
    return coef.reshape(local), res.reshape(local)


def solution(mesh):
    n = mesh.shape["pts"]
    return jax.shard_map(
        functools.partial(body, n), mesh=mesh,
        in_specs=(P("pts", None), P("pts"), P()),
        out_specs=(P("pts"), P("pts")), check_vma=False)
```

```python
import functools

import jax
import jax.numpy as jnp
from jax import lax
from jax.experimental import pallas as pl
from jax.experimental.pallas import tpu as pltpu
from jax.sharding import PartitionSpec as P

F32 = jnp.float32
BF16 = jnp.bfloat16
KEEP_BYTES = 40 * 1024 * 1024


def kernel(n, dim, keep, pts_hbm, tgt, ridge, coef_out, res_out, pts, blocks, t_all, w_all,
           c_all, r_a, r_b, kt, sem_in, sem_ps, sem_pr, sem_fs, sem_fr, sem_ws,
           sem_wr, sem_gs, sem_gr, sem_cs, sem_cr):
    me = lax.axis_index("pts")
    half_n = n // 2
    stages = half_n.bit_length() - 1
    local = tgt.shape[1]
    half = local // 2
    quarter = local // 4
    wide = 2 * dim
    t_rows = quarter // wide
    low = half_n // 4

    def device(p, q):
        d = lax.rem(me + p, 2)
        for s in range(stages):
            bit = half_n >> s
            d = d + lax.rem(me // bit + q // (1 << s), 2) * bit
        return d

    def stage_bit(z, s):
        if z and s >= stages - 2:
            s = 2 * stages - 3 - s
        return 1 << s

    def swapped(q):
        return q - low * (lax.rem(q // (2 * low), 2) - lax.rem(q // low, 2))

    partner = device(1, 0)
    load = pltpu.make_async_copy(pts_hbm, pts, sem_in)
    load.start()
    barrier = pltpu.get_barrier_semaphore()
    for dev in [partner] + [device(0, 1 << s) for s in range(stages)]:
        pl.semaphore_signal(barrier, inc=1, device_id=(dev,), device_id_type=pl.DeviceIdType.MESH)

    target = tgt[...]
    t_hi = target.astype(BF16)
    t_rest = target - t_hi.astype(F32)
    t_mid = t_rest.astype(BF16)
    t_lo = (t_rest - t_mid.astype(F32)).astype(BF16)
    parts = [part.astype(F32) for part in (t_hi, t_mid, t_lo)]

    def t_tile(z):
        cut = [part[:, i:i + wide] for part in parts for h in (0, half)
               for i in range(h + z * quarter, h + (z + 1) * quarter, wide)]
        pad = -len(cut) % 16
        return jnp.concatenate(cut + [jnp.zeros((pad, wide), F32)], axis=0).astype(BF16)

    load.wait()
    own = pts[...].astype(F32)
    packed = jnp.concatenate([own[:half], own[half:]], axis=1).astype(BF16)
    for z in (0, 1):
        blocks[0, 0, z, 0:quarter] = packed[z * quarter:(z + 1) * quarter]
        blocks[0, 0, z, quarter:] = t_tile(z)
    own_t = own.T
    s_row = jnp.sum(own_t * own_t, axis=0, keepdims=True) * (-1.0 / dim)
    s_hi = s_row.astype(BF16).astype(F32)
    s_mid = (s_row - s_hi).astype(BF16).astype(F32)
    s_lo = s_row - s_hi - s_mid
    rows = lax.broadcasted_iota(jnp.int32, (dim, local), 0)
    pieces = jnp.where(rows == 0, s_hi, jnp.where(rows == 1, s_mid, jnp.where(rows == 2, s_lo, 0.0)))
    pieces = pieces.astype(BF16)
    scaled = (own_t * (2.0 / dim)).astype(BF16)
    minus = jnp.full((dim, local), -1.0 / dim, BF16)
    r_a[0:dim] = scaled
    r_a[dim:2 * dim] = minus
    r_a[2 * dim:3 * dim] = minus
    r_a[3 * dim:4 * dim] = pieces
    r_b[0:dim] = minus
    r_b[dim:2 * dim] = scaled
    r_b[2 * dim:3 * dim] = pieces
    r_b[3 * dim:4 * dim] = minus

    def send(src, dst, ssem, rsem, dev):
        return pltpu.make_async_remote_copy(
            src_ref=src, dst_ref=dst, send_sem=ssem, recv_sem=rsem,
            device_id=(dev,), device_id_type=pl.DeviceIdType.MESH)

    def w_copy(q):
        return send(w_all.at[0, 0], w_all.at[0, q], sem_ws.at[q], sem_wr.at[q], device(0, q))

    def g_copy(q):
        return send(w_all.at[0, q], w_all.at[1, q], sem_gs.at[q], sem_gr.at[q], partner)

    def c_copy(p, q):
        return send(c_all.at[0, 0], c_all.at[p, q], sem_cs.at[p, q], sem_cr.at[p, q], device(p, q))

    def p_copy(z, q, s):
        to = q + (1 << s)
        return send(blocks.at[0, q, z], blocks.at[0, to, z], sem_ps.at[z, to], sem_pr.at[z, to],
                    device(0, stage_bit(z, s)))

    def p_from(z, q):
        return send(blocks.at[0, 0, z], blocks.at[0, q, z], sem_ps.at[z, q], sem_pr.at[z, q], partner)

    def f_copy(z, q):
        return send(blocks.at[0, q, z], blocks.at[1, q, z], sem_fs.at[z, q], sem_fr.at[z, q], partner)

    def each(fn):
        fn(1, 0)

        @pl.loop(1, half_n)
        def _(q):
            fn(0, q)
            fn(1, q)

    pl.semaphore_wait(barrier, stages + 1)
    for s in reversed(range(stages)):
        for z in (0, 1):
            p_copy(z, 0, s).start()
    for z in (0, 1):
        f_copy(z, 0).start()

    lanes = lax.broadcasted_iota(jnp.int32, (quarter, wide), 1)
    first = lanes < dim
    one = jnp.ones((quarter, wide), BF16)

    def tile(pb):
        f = pb.astype(F32)
        sq = f * f
        hi = sq.astype(BF16)
        lo = (sq - hi.astype(F32)).astype(BF16)
        hi = pltpu.roll(hi.astype(F32), dim, 1).astype(BF16)
        top = jnp.concatenate([jnp.where(first, pb, hi), jnp.where(first, lo, one)], axis=1)
        bot = jnp.concatenate([jnp.where(first, hi, pb), jnp.where(first, one, lo)], axis=1)
        e_top = jnp.dot(top, r_a[...], preferred_element_type=F32)
        k_top = jnp.exp(e_top).astype(BF16)
        e_bot = jnp.dot(bot, r_b[...], preferred_element_type=F32)
        k_bot = jnp.exp(e_bot).astype(BF16)
        return k_top, k_bot

    def at(z, h):
        return pl.ds(h * half + z * quarter, quarter)

    def absorb(p, q, vec_of, acc):
        for z in (0, 1):
            slot = swapped(q) if z else q
            k_top, k_bot = tile(blocks[p, q, z, 0:quarter])
            if keep:
                kt[p, slot, at(z, 0)] = k_top
                kt[p, slot, at(z, 1)] = k_bot
            v = jnp.concatenate(vec_of(p, q, z, slot), axis=1)
            acc = acc + jnp.dot(v, jnp.concatenate([k_top, k_bot], axis=0), preferred_element_type=F32)
        return acc

    def fresh(p, q, z, slot):
        part = blocks[p, q, z, quarter:].astype(F32)
        found = []
        for h in (0, 1):
            hi, mid, lo = (
                jnp.concatenate([part[(2 * i + h) * t_rows + j:(2 * i + h) * t_rows + j + 1] for j in range(t_rows)], axis=1)
                for i in range(3))
            t_all[p, slot, :, at(z, h)] = hi + mid + lo
            found.append(hi.astype(BF16))
        return found

    def stored(p, q, z, slot):
        return [t_all[p, slot, :, at(z, h)].astype(BF16) for h in (0, 1)]

    acc = absorb(0, 0, fresh, jnp.zeros((1, local), F32))

    def step(q, acc):
        for z in (0, 1):
            p_from(z, q).wait_recv()
            for s in reversed(range(stages)):
                @pl.when(q < (1 << s))
                def _():
                    p_copy(z, q, s).start()
            f_copy(z, q).start()
        for z in (0, 1):
            f_copy(z, q - 1).wait_recv()
        acc = absorb(0, q, fresh, acc)
        return absorb(1, q - 1, fresh, acc)

    acc = lax.fori_loop(1, half_n, step, acc)
    for z in (0, 1):
        f_copy(z, half_n - 1).wait_recv()
    acc = absorb(1, half_n - 1, fresh, acc)
    weight = ridge[0, 0]
    w_all[0, 0] = acc + weight * target
    t_whole = t_all[...]
    norm0 = jnp.sum(t_whole * t_whole)
    g_copy(0).start()

    @pl.loop(1, half_n)
    def _(q):
        w_copy(q).start()

    for z in (0, 1):
        f_copy(z, 0).wait_send()

    @pl.loop(1, half_n)
    def _(q):
        for z in (0, 1):
            p_from(z, q).wait_send()
            f_copy(z, q).wait_send()

    @pl.loop(1, half_n)
    def _(q):
        w_copy(q).wait_recv()
        g_copy(q).start()

    @pl.loop(1, half_n)
    def _(q):
        w_copy(q).wait_send()

    @pl.loop(0, half_n)
    def _(q):
        g_copy(q).wait()

    w_whole = w_all[...]
    step0 = norm0 / jnp.sum(t_whole * w_whole)
    r1 = t_whole - step0 * w_whole
    norm1 = jnp.sum(r1 * r1)
    d1 = r1 + (norm1 / norm0) * t_whole
    t_all[...] = d1

    def again(q, acc):
        for p in (0, 1):
            if keep:
                acc = acc + jnp.dot(t_all[p, q].astype(BF16), kt[p, q], preferred_element_type=F32)
            else:
                acc = absorb(p, q, stored, acc)
        return acc

    acc = lax.fori_loop(0, half_n, again, jnp.zeros((1, local), F32))
    d_own = t_all[0, 0]
    applied = acc + weight * d_own
    part = jnp.sum(d_own * applied)
    c_all[0, 0] = jnp.full((1, 128), part, F32)
    each(lambda p, q: c_copy(p, q).start())
    each(lambda p, q: c_copy(p, q).wait_recv())
    each(lambda p, q: c_copy(p, q).wait_send())
    curvature = jnp.sum(jnp.sum(c_all[...], axis=(0, 1)), axis=0, keepdims=True)[:, 0:1]
    step1 = norm1 / curvature
    coef_out[...] = step0 * target + step1 * d_own
    res_out[...] = target - step0 * w_all[0, 0] - step1 * applied


def body(n, points, targets, ridge_weight):
    local, dim = points.shape
    half_n = n // 2
    keep = n * local * local * 2 <= KEEP_BYTES
    kt_shape = (2, half_n, local, local) if keep else (1, 1, 16, 128)
    quarter = local // 4
    t_tile = -(-6 * quarter // (32 * dim)) * 16
    dma = pltpu.SemaphoreType.DMA
    vec = jax.ShapeDtypeStruct((1, local), F32)
    coef, res = pl.pallas_call(
        functools.partial(kernel, n, dim, keep),
        out_shape=(vec, vec),
        in_specs=[
            pl.BlockSpec(memory_space=pl.ANY),
            pl.BlockSpec(memory_space=pltpu.VMEM),
            pl.BlockSpec(memory_space=pltpu.SMEM),
        ],
        out_specs=(pl.BlockSpec(memory_space=pltpu.VMEM), pl.BlockSpec(memory_space=pltpu.VMEM)),
        scratch_shapes=[
            pltpu.VMEM((local, dim), BF16),
            pltpu.VMEM((2, half_n, 2, quarter + t_tile, 2 * dim), BF16),
            pltpu.VMEM((2, half_n, 1, local), F32),
            pltpu.VMEM((2, half_n, 1, local), F32),
            pltpu.VMEM((2, half_n, 1, 128), F32),
            pltpu.VMEM((4 * dim, local), BF16),
            pltpu.VMEM((4 * dim, local), BF16),
            pltpu.VMEM(kt_shape, BF16),
            dma,
            dma((2, half_n)), dma((2, half_n)),
            dma((2, half_n)), dma((2, half_n)),
            dma((half_n,)), dma((half_n,)),
            dma((half_n,)), dma((half_n,)),
            dma((2, half_n)), dma((2, half_n)),
        ],
        compiler_params=pltpu.CompilerParams(
            collective_id=0, has_side_effects=True, vmem_limit_bytes=60 * 1024 * 1024),
    )(points, targets.reshape(1, local), ridge_weight.reshape(1, 1))
    return coef.reshape(local), res.reshape(local)


def solution(mesh):
    n = mesh.shape["pts"]
    return jax.shard_map(
        functools.partial(body, n), mesh=mesh,
        in_specs=(P("pts", None), P("pts"), P()),
        out_specs=(P("pts"), P("pts")), check_vma=False)
```

```python
import functools

import jax
import jax.numpy as jnp
from jax import lax
from jax.experimental import pallas as pl
from jax.experimental.pallas import tpu as pltpu
from jax.sharding import PartitionSpec as P

F32 = jnp.float32
BF16 = jnp.bfloat16
KEEP_BYTES = 40 * 1024 * 1024


def kernel(n, dim, keep, pts_hbm, tgt, ridge, coef_out, res_out, pts, blocks, t_all, w_all,
           c_all, r_a, r_b, kt, sem_in, sem_ps, sem_pr, sem_fs, sem_fr, sem_ws,
           sem_wr, sem_gs, sem_gr, sem_cs, sem_cr):
    me = lax.axis_index("pts")
    half_n = n // 2
    stages = half_n.bit_length() - 1
    local = tgt.shape[1]
    half = local // 2
    quarter = local // 4
    wide = 2 * dim
    t_rows = quarter // wide
    low = half_n // 4

    def device(p, q):
        d = lax.rem(me + p, 2)
        for s in range(stages):
            bit = half_n >> (s if s >= stages - 2 else stages - 3 - s)
            d = d + lax.rem(me // bit + q // (1 << s), 2) * bit
        return d

    def stage_bit(z, s):
        if z and s >= stages - 2:
            s = 2 * stages - 3 - s
        return 1 << s

    def swapped(q):
        return q - low * (lax.rem(q // (2 * low), 2) - lax.rem(q // low, 2))

    def turn(i):
        q = jnp.where(i - 1 < 2 * low, i - 1, i)
        q = jnp.where(i - 2 < low, i - 2, q)
        return jnp.where(i == 0, 0, jnp.where(i == 1, low, jnp.where(i == 2, 2 * low, q)))

    partner = device(1, 0)
    load = pltpu.make_async_copy(pts_hbm, pts, sem_in)
    load.start()
    barrier = pltpu.get_barrier_semaphore()
    for dev in [partner, device(0, 3)] + [device(0, 1 << s) for s in range(stages)]:
        pl.semaphore_signal(barrier, inc=1, device_id=(dev,), device_id_type=pl.DeviceIdType.MESH)

    target = tgt[...]
    t_hi = target.astype(BF16)
    t_rest = target - t_hi.astype(F32)
    t_mid = t_rest.astype(BF16)
    t_lo = (t_rest - t_mid.astype(F32)).astype(BF16)
    parts = [part.astype(F32) for part in (t_hi, t_mid, t_lo)]

    def t_tile(z):
        cut = [part[:, i:i + wide] for part in parts for h in (0, half)
               for i in range(h + z * quarter, h + (z + 1) * quarter, wide)]
        pad = -len(cut) % 16
        return jnp.concatenate(cut + [jnp.zeros((pad, wide), F32)], axis=0).astype(BF16)

    load.wait()
    own = pts[...].astype(F32)
    packed = jnp.concatenate([own[:half], own[half:]], axis=1).astype(BF16)
    for z in (0, 1):
        blocks[0, 0, z, 0:quarter] = packed[z * quarter:(z + 1) * quarter]
        blocks[0, 0, z, quarter:] = t_tile(z)
    own_t = own.T
    s_row = jnp.sum(own_t * own_t, axis=0, keepdims=True) * (-1.0 / dim)
    s_hi = s_row.astype(BF16).astype(F32)
    s_mid = (s_row - s_hi).astype(BF16).astype(F32)
    s_lo = s_row - s_hi - s_mid
    rows = lax.broadcasted_iota(jnp.int32, (dim, local), 0)
    pieces = jnp.where(rows == 0, s_hi, jnp.where(rows == 1, s_mid, jnp.where(rows == 2, s_lo, 0.0)))
    pieces = pieces.astype(BF16)
    scaled = (own_t * (2.0 / dim)).astype(BF16)
    minus = jnp.full((dim, local), -1.0 / dim, BF16)
    r_a[0:dim] = scaled
    r_a[dim:2 * dim] = minus
    r_a[2 * dim:3 * dim] = minus
    r_a[3 * dim:4 * dim] = pieces
    r_b[0:dim] = minus
    r_b[dim:2 * dim] = scaled
    r_b[2 * dim:3 * dim] = pieces
    r_b[3 * dim:4 * dim] = minus

    def send(src, dst, ssem, rsem, dev):
        return pltpu.make_async_remote_copy(
            src_ref=src, dst_ref=dst, send_sem=ssem, recv_sem=rsem,
            device_id=(dev,), device_id_type=pl.DeviceIdType.MESH)

    def w_copy(q):
        return send(w_all.at[0, 0], w_all.at[0, q], sem_ws.at[q], sem_wr.at[q], device(0, q))

    def g_copy(q):
        return send(w_all.at[0, q], w_all.at[1, q], sem_gs.at[q], sem_gr.at[q], partner)

    def c_copy(p, q):
        return send(c_all.at[0, 0], c_all.at[p, q], sem_cs.at[p, q], sem_cr.at[p, q], device(p, q))

    def p_copy(z, q, s):
        to = q + (1 << s)
        return send(blocks.at[0, q, z], blocks.at[0, to, z], sem_ps.at[z, to], sem_pr.at[z, to],
                    device(0, stage_bit(z, s)))

    def p_from(z, q):
        return send(blocks.at[0, 0, z], blocks.at[0, q, z], sem_ps.at[z, q], sem_pr.at[z, q], partner)

    def f_copy(z, q):
        return send(blocks.at[0, q, z], blocks.at[1, q, z], sem_fs.at[z, q], sem_fr.at[z, q], partner)

    def each(fn):
        fn(1, 0)

        @pl.loop(1, half_n)
        def _(q):
            fn(0, q)
            fn(1, q)

    pl.semaphore_wait(barrier, stages + 2)
    for s in reversed(range(stages)):
        for z in (0, 1):
            p_copy(z, 0, s).start()
    for z in (0, 1):
        send(blocks.at[0, 0, z], blocks.at[0, 3, z], sem_ps.at[z, 3], sem_pr.at[z, 3], device(0, 3)).start()
    for z in (0, 1):
        f_copy(z, 0).start()

    lanes = lax.broadcasted_iota(jnp.int32, (quarter, wide), 1)
    first = lanes < dim
    one = jnp.ones((quarter, wide), BF16)

    def tile(pb):
        f = pb.astype(F32)
        sq = f * f
        hi = sq.astype(BF16)
        lo = (sq - hi.astype(F32)).astype(BF16)
        hi = pltpu.roll(hi.astype(F32), dim, 1).astype(BF16)
        top = jnp.concatenate([jnp.where(first, pb, hi), jnp.where(first, lo, one)], axis=1)
        bot = jnp.concatenate([jnp.where(first, hi, pb), jnp.where(first, one, lo)], axis=1)
        return top, bot

    def at(z, h):
        return pl.ds(h * half + z * quarter, quarter)

    def absorb(p, q, vec_of, acc):
        slots = (q, swapped(q))
        tiles = [tile(blocks[p, q, z, 0:quarter]) for z in (0, 1)]
        vecs = [vec_of(p, q, z, slots[z]) for z in (0, 1)]
        for h in (0, 1):
            both = jnp.concatenate([tiles[0][h], tiles[1][h]], axis=0)
            e = jnp.dot(both, (r_a, r_b)[h][...], preferred_element_type=F32)
            k = jnp.exp(e).astype(BF16)
            if keep:
                for z in (0, 1):
                    kt[p, slots[z], at(z, h)] = k[z * quarter:(z + 1) * quarter]
            v = jnp.concatenate([vecs[0][h], vecs[1][h]], axis=1)
            acc = acc + jnp.dot(v, k, preferred_element_type=F32)
        return acc

    def fresh(p, q, z, slot):
        part = blocks[p, q, z, quarter:].astype(F32)
        found = []
        for h in (0, 1):
            hi, mid, lo = (
                jnp.concatenate([part[(2 * i + h) * t_rows + j:(2 * i + h) * t_rows + j + 1] for j in range(t_rows)], axis=1)
                for i in range(3))
            t_all[p, slot, :, at(z, h)] = hi + mid + lo
            found.append(hi.astype(BF16))
        return found

    def stored(p, q, z, slot):
        return [t_all[p, slot, :, at(z, h)].astype(BF16) for h in (0, 1)]

    acc = absorb(0, 0, fresh, jnp.zeros((1, local), F32))

    def step(i, acc):
        q = turn(i)
        last = turn(i - 1)
        for z in (0, 1):
            p_from(z, q).wait_recv()
            for s in reversed(range(2, stages)):
                @pl.when(q < (1 << s))
                def _():
                    p_copy(z, q, s).start()
            f_copy(z, q).start()
        for z in (0, 1):
            f_copy(z, last).wait_recv()
        acc = absorb(0, q, fresh, acc)
        return absorb(1, last, fresh, acc)

    acc = lax.fori_loop(1, half_n, step, acc)
    for z in (0, 1):
        f_copy(z, half_n - 1).wait_recv()
    acc = absorb(1, half_n - 1, fresh, acc)
    weight = ridge[0, 0]
    w_all[0, 0] = acc + weight * target
    t_whole = t_all[...]
    norm0 = jnp.sum(t_whole * t_whole)
    g_copy(0).start()

    @pl.loop(1, half_n)
    def _(q):
        w_copy(q).start()

    for z in (0, 1):
        f_copy(z, 0).wait_send()

    @pl.loop(1, half_n)
    def _(q):
        for z in (0, 1):
            p_from(z, q).wait_send()
            f_copy(z, q).wait_send()

    @pl.loop(1, half_n)
    def _(q):
        w_copy(q).wait_recv()
        g_copy(q).start()

    @pl.loop(1, half_n)
    def _(q):
        w_copy(q).wait_send()

    @pl.loop(0, half_n)
    def _(q):
        g_copy(q).wait()

    w_whole = w_all[...]
    step0 = norm0 / jnp.sum(t_whole * w_whole)
    r1 = t_whole - step0 * w_whole
    norm1 = jnp.sum(r1 * r1)
    d1 = r1 + (norm1 / norm0) * t_whole
    t_all[...] = d1

    def again(q, acc):
        for p in (0, 1):
            if keep:
                acc = acc + jnp.dot(t_all[p, q].astype(BF16), kt[p, q], preferred_element_type=F32)
            else:
                acc = absorb(p, q, stored, acc)
        return acc

    acc = lax.fori_loop(0, half_n, again, jnp.zeros((1, local), F32))
    d_own = t_all[0, 0]
    applied = acc + weight * d_own
    part = jnp.sum(d_own * applied)
    c_all[0, 0] = jnp.full((1, 128), part, F32)
    each(lambda p, q: c_copy(p, q).start())
    each(lambda p, q: c_copy(p, q).wait_recv())
    each(lambda p, q: c_copy(p, q).wait_send())
    curvature = jnp.sum(jnp.sum(c_all[...], axis=(0, 1)), axis=0, keepdims=True)[:, 0:1]
    step1 = norm1 / curvature
    coef_out[...] = step0 * target + step1 * d_own
    res_out[...] = target - step0 * w_all[0, 0] - step1 * applied


def body(n, points, targets, ridge_weight):
    local, dim = points.shape
    half_n = n // 2
    keep = n * local * local * 2 <= KEEP_BYTES
    kt_shape = (2, half_n, local, local) if keep else (1, 1, 16, 128)
    quarter = local // 4
    t_tile = -(-6 * quarter // (32 * dim)) * 16
    dma = pltpu.SemaphoreType.DMA
    vec = jax.ShapeDtypeStruct((1, local), F32)
    coef, res = pl.pallas_call(
        functools.partial(kernel, n, dim, keep),
        out_shape=(vec, vec),
        in_specs=[
            pl.BlockSpec(memory_space=pl.ANY),
            pl.BlockSpec(memory_space=pltpu.VMEM),
            pl.BlockSpec(memory_space=pltpu.SMEM),
        ],
        out_specs=(pl.BlockSpec(memory_space=pltpu.VMEM), pl.BlockSpec(memory_space=pltpu.VMEM)),
        scratch_shapes=[
            pltpu.VMEM((local, dim), BF16),
            pltpu.VMEM((2, half_n, 2, quarter + t_tile, 2 * dim), BF16),
            pltpu.VMEM((2, half_n, 1, local), F32),
            pltpu.VMEM((2, half_n, 1, local), F32),
            pltpu.VMEM((2, half_n, 1, 128), F32),
            pltpu.VMEM((4 * dim, local), BF16),
            pltpu.VMEM((4 * dim, local), BF16),
            pltpu.VMEM(kt_shape, BF16),
            dma,
            dma((2, half_n)), dma((2, half_n)),
            dma((2, half_n)), dma((2, half_n)),
            dma((half_n,)), dma((half_n,)),
            dma((half_n,)), dma((half_n,)),
            dma((2, half_n)), dma((2, half_n)),
        ],
        compiler_params=pltpu.CompilerParams(
            collective_id=0, has_side_effects=True, vmem_limit_bytes=60 * 1024 * 1024),
    )(points, targets.reshape(1, local), ridge_weight.reshape(1, 1))
    return coef.reshape(local), res.reshape(local)


def solution(mesh):
    n = mesh.shape["pts"]
    return jax.shard_map(
        functools.partial(body, n), mesh=mesh,
        in_specs=(P("pts", None), P("pts"), P()),
        out_specs=(P("pts"), P("pts")), check_vma=False)
```

```python
import functools

import jax
import jax.numpy as jnp
from jax import lax
from jax.experimental import pallas as pl
from jax.experimental.pallas import tpu as pltpu
from jax.sharding import PartitionSpec as P

F32 = jnp.float32
BF16 = jnp.bfloat16
KEEP_BYTES = 40 * 1024 * 1024


def kernel(n, dim, keep, pts_hbm, tgt, ridge, coef_out, res_out, pts, blocks, t_all, w_all,
           c_all, r_a, r_b, kt, sem_in, sem_ps, sem_pr, sem_fs, sem_fr, sem_ws,
           sem_wr, sem_gs, sem_gr, sem_cs, sem_cr):
    me = lax.axis_index("pts")
    half_n = n // 2
    stages = half_n.bit_length() - 1
    local = tgt.shape[1]
    half = local // 2
    quarter = local // 4
    wide = 2 * dim
    t_rows = quarter // wide
    low = half_n // 4

    def device(p, q):
        d = lax.rem(me + p, 2)
        for s in range(stages):
            bit = half_n >> (s if s >= stages - 2 else stages - 3 - s)
            d = d + lax.rem(me // bit + q // (1 << s), 2) * bit
        return d

    def stage_bit(z, s):
        if z and s >= stages - 2:
            s = 2 * stages - 3 - s
        return 1 << s

    def swapped(q):
        return q - low * (lax.rem(q // (2 * low), 2) - lax.rem(q // low, 2))

    def turn(i):
        q = jnp.where(i - 1 < 2 * low, i - 1, i)
        q = jnp.where(i - 2 < low, i - 2, q)
        return jnp.where(i == 0, 0, jnp.where(i == 1, low, jnp.where(i == 2, 2 * low, q)))

    partner = device(1, 0)
    load = pltpu.make_async_copy(pts_hbm, pts, sem_in)
    load.start()
    barrier = pltpu.get_barrier_semaphore()
    for dev in [partner, device(0, 3)] + [device(0, 1 << s) for s in range(stages)]:
        pl.semaphore_signal(barrier, inc=1, device_id=(dev,), device_id_type=pl.DeviceIdType.MESH)

    target = tgt[...]
    t_hi = target.astype(BF16)
    t_rest = target - t_hi.astype(F32)
    t_mid = t_rest.astype(BF16)
    t_lo = (t_rest - t_mid.astype(F32)).astype(BF16)
    parts = [part.astype(F32) for part in (t_hi, t_mid, t_lo)]

    def t_tile(z):
        cut = [part[:, i:i + wide] for part in parts for h in (0, half)
               for i in range(h + z * quarter, h + (z + 1) * quarter, wide)]
        pad = -len(cut) % 16
        return jnp.concatenate(cut + [jnp.zeros((pad, wide), F32)], axis=0).astype(BF16)

    load.wait()
    own = pts[...].astype(F32)
    packed = jnp.concatenate([own[:half], own[half:]], axis=1).astype(BF16)
    for z in (0, 1):
        blocks[0, 0, z, 0:quarter] = packed[z * quarter:(z + 1) * quarter]
        blocks[0, 0, z, quarter:] = t_tile(z)
    own_t = own.T
    s_row = jnp.sum(own_t * own_t, axis=0, keepdims=True) * (-1.0 / dim)
    s_hi = s_row.astype(BF16).astype(F32)
    s_mid = (s_row - s_hi).astype(BF16).astype(F32)
    s_lo = s_row - s_hi - s_mid
    rows = lax.broadcasted_iota(jnp.int32, (dim, local), 0)
    pieces = jnp.where(rows == 0, s_hi, jnp.where(rows == 1, s_mid, jnp.where(rows == 2, s_lo, 0.0)))
    pieces = pieces.astype(BF16)
    scaled = (own_t * (2.0 / dim)).astype(BF16)
    minus = jnp.full((dim, local), -1.0 / dim, BF16)
    r_a[0:dim] = scaled
    r_a[dim:2 * dim] = minus
    r_a[2 * dim:3 * dim] = minus
    r_a[3 * dim:4 * dim] = pieces
    r_b[0:dim] = minus
    r_b[dim:2 * dim] = scaled
    r_b[2 * dim:3 * dim] = pieces
    r_b[3 * dim:4 * dim] = minus

    def send(src, dst, ssem, rsem, dev):
        return pltpu.make_async_remote_copy(
            src_ref=src, dst_ref=dst, send_sem=ssem, recv_sem=rsem,
            device_id=(dev,), device_id_type=pl.DeviceIdType.MESH)

    def w_copy(q):
        return send(w_all.at[0, 0], w_all.at[0, q], sem_ws.at[q], sem_wr.at[q], device(0, q))

    def g_copy(q):
        return send(w_all.at[0, q], w_all.at[1, q], sem_gs.at[q], sem_gr.at[q], partner)

    def c_copy(p, q):
        return send(c_all.at[0, 0], c_all.at[p, q], sem_cs.at[p, q], sem_cr.at[p, q], device(p, q))

    def p_copy(z, q, s):
        to = q + (1 << s)
        return send(blocks.at[0, q, z], blocks.at[0, to, z], sem_ps.at[z, to], sem_pr.at[z, to],
                    device(0, stage_bit(z, s)))

    def p_from(z, q):
        return send(blocks.at[0, 0, z], blocks.at[0, q, z], sem_ps.at[z, q], sem_pr.at[z, q], partner)

    def f_copy(z, q):
        return send(blocks.at[0, q, z], blocks.at[1, q, z], sem_fs.at[z, q], sem_fr.at[z, q], partner)

    def each(fn):
        fn(1, 0)

        @pl.loop(1, half_n)
        def _(q):
            fn(0, q)
            fn(1, q)

    pl.semaphore_wait(barrier, stages + 2)
    for z in (0, 1):
        send(blocks.at[0, 0, z], blocks.at[0, 3, z], sem_ps.at[z, 3], sem_pr.at[z, 3], device(0, 3)).start()
    for s in range(stages):
        for z in (0, 1):
            p_copy(z, 0, s).start()
    for z in (0, 1):
        f_copy(z, 0).start()

    lanes = lax.broadcasted_iota(jnp.int32, (quarter, wide), 1)
    first = lanes < dim
    one = jnp.ones((quarter, wide), BF16)

    def tile(pb):
        f = pb.astype(F32)
        sq = f * f
        hi = sq.astype(BF16)
        lo = (sq - hi.astype(F32)).astype(BF16)
        hi = pltpu.roll(hi.astype(F32), dim, 1).astype(BF16)
        top = jnp.concatenate([jnp.where(first, pb, hi), jnp.where(first, lo, one)], axis=1)
        bot = jnp.concatenate([jnp.where(first, hi, pb), jnp.where(first, one, lo)], axis=1)
        return top, bot

    def at(z, h):
        return pl.ds(h * half + z * quarter, quarter)

    def absorb(p, q, vec_of, acc):
        slots = (q, swapped(q))
        tiles = [tile(blocks[p, q, z, 0:quarter]) for z in (0, 1)]
        vecs = [vec_of(p, q, z, slots[z]) for z in (0, 1)]
        for h in (0, 1):
            both = jnp.concatenate([tiles[0][h], tiles[1][h]], axis=0)
            e = jnp.dot(both, (r_a, r_b)[h][...], preferred_element_type=F32)
            k = jnp.exp(e).astype(BF16)
            if keep:
                for z in (0, 1):
                    kt[p, slots[z], at(z, h)] = k[z * quarter:(z + 1) * quarter]
            v = jnp.concatenate([vecs[0][h], vecs[1][h]], axis=1)
            acc = acc + jnp.dot(v, k, preferred_element_type=F32)
        return acc

    def fresh(p, q, z, slot):
        part = blocks[p, q, z, quarter:].astype(F32)
        found = []
        for h in (0, 1):
            hi, mid, lo = (
                jnp.concatenate([part[(2 * i + h) * t_rows + j:(2 * i + h) * t_rows + j + 1] for j in range(t_rows)], axis=1)
                for i in range(3))
            t_all[p, slot, :, at(z, h)] = hi + mid + lo
            found.append(hi.astype(BF16))
        return found

    def stored(p, q, z, slot):
        return [t_all[p, slot, :, at(z, h)].astype(BF16) for h in (0, 1)]

    acc = absorb(0, 0, fresh, jnp.zeros((1, local), F32))

    def step(i, acc):
        q = turn(i)
        last = turn(i - 1)
        for z in (0, 1):
            p_from(z, q).wait_recv()
            for s in reversed(range(2, stages)):
                @pl.when(q < (1 << s))
                def _():
                    p_copy(z, q, s).start()
            f_copy(z, q).start()
        for z in (0, 1):
            f_copy(z, last).wait_recv()
        acc = absorb(0, q, fresh, acc)
        return absorb(1, last, fresh, acc)

    acc = lax.fori_loop(1, half_n, step, acc)
    for z in (0, 1):
        f_copy(z, half_n - 1).wait_recv()
    acc = absorb(1, half_n - 1, fresh, acc)
    weight = ridge[0, 0]
    w_all[0, 0] = acc + weight * target
    t_whole = t_all[...]
    norm0 = jnp.sum(t_whole * t_whole)
    g_copy(0).start()

    @pl.loop(1, half_n)
    def _(q):
        w_copy(q).start()

    for z in (0, 1):
        f_copy(z, 0).wait_send()

    @pl.loop(1, half_n)
    def _(q):
        for z in (0, 1):
            p_from(z, q).wait_send()
            f_copy(z, q).wait_send()

    @pl.loop(1, half_n)
    def _(q):
        w_copy(q).wait_recv()
        g_copy(q).start()

    @pl.loop(1, half_n)
    def _(q):
        w_copy(q).wait_send()

    @pl.loop(0, half_n)
    def _(q):
        g_copy(q).wait()

    w_whole = w_all[...]
    step0 = norm0 / jnp.sum(t_whole * w_whole)
    r1 = t_whole - step0 * w_whole
    norm1 = jnp.sum(r1 * r1)
    d1 = r1 + (norm1 / norm0) * t_whole
    t_all[...] = d1

    def again(q, acc):
        for p in (0, 1):
            if keep:
                acc = acc + jnp.dot(t_all[p, q].astype(BF16), kt[p, q], preferred_element_type=F32)
            else:
                acc = absorb(p, q, stored, acc)
        return acc

    acc = lax.fori_loop(0, half_n, again, jnp.zeros((1, local), F32))
    d_own = t_all[0, 0]
    applied = acc + weight * d_own
    part = jnp.sum(d_own * applied)
    c_all[0, 0] = jnp.full((1, 128), part, F32)
    each(lambda p, q: c_copy(p, q).start())
    each(lambda p, q: c_copy(p, q).wait_recv())
    each(lambda p, q: c_copy(p, q).wait_send())
    curvature = jnp.sum(jnp.sum(c_all[...], axis=(0, 1)), axis=0, keepdims=True)[:, 0:1]
    step1 = norm1 / curvature
    coef_out[...] = step0 * target + step1 * d_own
    res_out[...] = target - step0 * w_all[0, 0] - step1 * applied


def body(n, points, targets, ridge_weight):
    local, dim = points.shape
    half_n = n // 2
    keep = n * local * local * 2 <= KEEP_BYTES
    kt_shape = (2, half_n, local, local) if keep else (1, 1, 16, 128)
    quarter = local // 4
    t_tile = -(-6 * quarter // (32 * dim)) * 16
    dma = pltpu.SemaphoreType.DMA
    vec = jax.ShapeDtypeStruct((1, local), F32)
    coef, res = pl.pallas_call(
        functools.partial(kernel, n, dim, keep),
        out_shape=(vec, vec),
        in_specs=[
            pl.BlockSpec(memory_space=pl.ANY),
            pl.BlockSpec(memory_space=pltpu.VMEM),
            pl.BlockSpec(memory_space=pltpu.SMEM),
        ],
        out_specs=(pl.BlockSpec(memory_space=pltpu.VMEM), pl.BlockSpec(memory_space=pltpu.VMEM)),
        scratch_shapes=[
            pltpu.VMEM((local, dim), BF16),
            pltpu.VMEM((2, half_n, 2, quarter + t_tile, 2 * dim), BF16),
            pltpu.VMEM((2, half_n, 1, local), F32),
            pltpu.VMEM((2, half_n, 1, local), F32),
            pltpu.VMEM((2, half_n, 1, 128), F32),
            pltpu.VMEM((4 * dim, local), BF16),
            pltpu.VMEM((4 * dim, local), BF16),
            pltpu.VMEM(kt_shape, BF16),
            dma,
            dma((2, half_n)), dma((2, half_n)),
            dma((2, half_n)), dma((2, half_n)),
            dma((half_n,)), dma((half_n,)),
            dma((half_n,)), dma((half_n,)),
            dma((2, half_n)), dma((2, half_n)),
        ],
        compiler_params=pltpu.CompilerParams(
            collective_id=0, has_side_effects=True, vmem_limit_bytes=60 * 1024 * 1024),
    )(points, targets.reshape(1, local), ridge_weight.reshape(1, 1))
    return coef.reshape(local), res.reshape(local)


def solution(mesh):
    n = mesh.shape["pts"]
    return jax.shard_map(
        functools.partial(body, n), mesh=mesh,
        in_specs=(P("pts", None), P("pts"), P()),
        out_specs=(P("pts"), P("pts")), check_vma=False)
```
